32 devices in a mesh: frag: 2 (over x), grid: 16 (over z, y, core).
Axes of the slice: x: 2, y: 2, z: 4, core: 2. Of those that a mesh axis runs over, the one named last changes fastest.
Arguments:
- psi: float32 [16384, 640], P(('frag', 'grid')), parts along dimension 0
- order: int32 [10], P('frag'), parts along dimension 0, may hold values from 0 to 4, each once
Outputs:
- orthonormal: float32 [16384, 640], P(('frag', 'grid')), parts along dimension 0
The draws below stay inside these ranges and needn't reach their ends.
There are 2 independent parts, one for each index of `frag`. The reference program is written for one: setup_inputs(seed, part) draws one part's arguments, and reference() takes and returns one part's arrays. A program takes and returns all parts, laid end to end along the dimension named above; each array names one. Nothing has to cross between parts.
All inputs are finite; a program needn't handle non-finite values.
Results may differ from the reference program's by a relative error of at most 0.00012.
Values sent between devices are 32-bit elements; how exact they have to be, the bound alone decides.
A program may use at most 64 MiB of HBM per device.

```python
import jax
import jax.numpy as jnp
from jax import lax

BLOCK = 128
NBLK = 5
BANDS = 640
POINTS = 8192


def draw_psi(key, part):
    own = jax.random.normal(jax.random.fold_in(key, 11), (POINTS, BANDS), jnp.float32)
    shared = jax.random.normal(jax.random.fold_in(key, 12), (POINTS, BLOCK), jnp.float32)
    mixed = own + 0.8 * jnp.tile(shared, (1, NBLK))
    return mixed.astype(jnp.float32)


def setup_inputs(seed: int = 0, part: int = 0) -> dict:
    streams_of = jax.random.split(jax.random.key(seed), 3)
    part_splits = jax.random.split(jax.random.fold_in(streams_of[2], part), 3)
    psi = draw_psi(jax.random.fold_in(jax.random.fold_in(streams_of[2], part), 71), part)
    order = jax.random.permutation(part_splits[1], NBLK).astype(jnp.int32)
    return {"psi": psi, "order": order}


def contract(left, right):
    return lax.dot_general(left.astype(jnp.float32), right.astype(jnp.float32), (((0,), (0,)), ((), ())), precision=lax.Precision.HIGHEST, preferred_element_type=jnp.float32)

def matmul(left, right):
    return jnp.dot(left.astype(jnp.float32), right.astype(jnp.float32), precision=lax.Precision.HIGHEST, preferred_element_type=jnp.float32)

def reference(psi, order):
    scale = jnp.float32(1.0 / POINTS)
    result = jnp.zeros_like(psi)
    done = []
    for step in range(NBLK):
        start = (order[step] * BLOCK).astype(jnp.int32)
        block = lax.dynamic_slice_in_dim(psi, start, BLOCK, 1)
        if step > 0:
            prev = jnp.concatenate(done, axis=1)
            coeff = contract(prev, block) * scale
            block = block - matmul(prev, coeff)
        gram = contract(block, block) * scale
        lower = jnp.linalg.cholesky(gram)
        inverse = lax.linalg.triangular_solve(lower, jnp.eye(BLOCK, dtype=gram.dtype), left_side=True, lower=True)
        basis = matmul(block, inverse.T)
        done.append(basis)
        result = lax.dynamic_update_slice(result, basis, (jnp.int32(0), start))
    return result
```

```python
import functools

import jax
import jax.numpy as jnp
from jax import lax
from jax.experimental import pallas as pl
from jax.experimental.pallas import tpu as pltpu
from jax.sharding import PartitionSpec as P

BLOCK = 128
PANEL = 16
TILE = 8
HIGHEST = lax.Precision.HIGHEST


def dot(left, right, dims):
    return lax.dot_general(
        left, right, (dims, ((), ())), precision=HIGHEST, preferred_element_type=jnp.float32
    )


def pairs(count):
    return [(i, j) for i in range(count) for j in range(i, count)]


def slot(i, j, count):
    return i * count - (i * (i - 1)) // 2 + (j - i)


def gram_kernel(bits, scale, psi_ref, out_ref, part, acc, recv, full, send_sem, recv_sem):
    me = lax.axis_index("grid")
    partners = [me + (1 - 2 * ((me // 2**k) % 2)) * 2**k for k in range(bits)]
    rows = part.shape[0]
    count = psi_ref.shape[1] // BLOCK

    barrier = pltpu.get_barrier_semaphore()
    for partner in partners:
        pl.semaphore_signal(
            barrier, inc=1, device_id={"grid": partner}, device_id_type=pl.DeviceIdType.MESH
        )

    at = 0
    for i in range(count):
        left = psi_ref[:, i * BLOCK : (i + 1) * BLOCK]
        row = dot(left, psi_ref[:, i * BLOCK :], ((0,), (0,))) * scale
        for j in range(i, count):
            part[at : at + BLOCK, :] = row[:, (j - i) * BLOCK : (j - i + 1) * BLOCK]
            at += BLOCK
    if at < rows:
        part[at:, :] = jnp.zeros((rows - at, BLOCK), jnp.float32)
    pl.semaphore_wait(barrier, bits)

    def send(src, dst, index, partner):
        copy = pltpu.make_async_remote_copy(
            src_ref=src,
            dst_ref=dst,
            send_sem=send_sem.at[index],
            recv_sem=recv_sem.at[index],
            device_id={"grid": partner},
            device_id_type=pl.DeviceIdType.MESH,
        )
        copy.start()
        return copy

    offset, size, base = 0, rows, 0
    for k in range(bits):
        size //= 2
        bit = (me // 2**k) % 2
        keep = pl.multiple_of(offset + bit * size, TILE)
        give = pl.multiple_of(offset + (1 - bit) * size, TILE)
        source = part if k == 0 else acc
        landing = recv.at[pl.ds(base, size)]
        send(source.at[pl.ds(give, size)], landing, k, partners[k]).wait()
        total = source[pl.ds(keep, size), :] + recv[base : base + size, :]
        if k == bits - 1:
            full[pl.ds(keep, size), :] = total
        else:
            acc[pl.ds(keep, size), :] = total
        offset, base = keep, base + size

    for k in reversed(range(bits)):
        bit = (me // 2**k) % 2
        here = full.at[pl.ds(pl.multiple_of(offset, TILE), size)]
        send(here, here, bits + k, partners[k]).wait()
        offset = offset - bit * size
        size *= 2
    out_ref[...] = full[: out_ref.shape[0], :]


def packed_gram(psi, devices):
    points, bands = psi.shape
    count = bands // BLOCK
    used = len(pairs(count)) * BLOCK
    chunk = -(-used // (devices * TILE)) * TILE
    rows = chunk * devices
    bits = devices.bit_length() - 1
    scale = float(1.0 / (points * devices))
    return pl.pallas_call(
        functools.partial(gram_kernel, bits, scale),
        out_shape=jax.ShapeDtypeStruct((used, BLOCK), jnp.float32),
        in_specs=[pl.BlockSpec(memory_space=pltpu.VMEM)],
        out_specs=pl.BlockSpec(memory_space=pltpu.VMEM),
        scratch_shapes=[
            pltpu.VMEM((rows, BLOCK), jnp.float32),
            pltpu.VMEM((rows, BLOCK), jnp.float32),
            pltpu.VMEM((rows, BLOCK), jnp.float32),
            pltpu.VMEM((rows, BLOCK), jnp.float32),
            pltpu.SemaphoreType.DMA((2 * bits,)),
            pltpu.SemaphoreType.DMA((2 * bits,)),
        ],
        compiler_params=pltpu.CompilerParams(collective_id=0, has_side_effects=True),
    )(psi)


def factor_block(gram):
    tiles = PANEL // TILE
    row = lax.broadcasted_iota(jnp.int32, (TILE, BLOCK), 0)
    lane = lax.broadcasted_iota(jnp.int32, (TILE, BLOCK), 1)
    rest, done = gram, []
    for start in range(0, BLOCK, PANEL):
        panel = [rest[r * TILE : (r + 1) * TILE, :] for r in range(tiles)]
        columns = [
            [jnp.broadcast_to(panel[r][:, start + j : start + j + 1], (TILE, BLOCK)) for r in range(tiles)]
            for j in range(PANEL)
        ]
        inside = (lane >= start) & (lane < start + PANEL)
        panel = [
            jnp.where(inside, jnp.where(lane == row + (start + r * TILE), 1.0, 0.0), panel[r])
            for r in range(tiles)
        ]
        pivots = [jnp.ones((TILE, BLOCK), jnp.float32)] * tiles
        for j in range(PANEL):
            own, sub = divmod(j, TILE)
            pivot = jnp.broadcast_to(columns[j][own][sub : sub + 1, :], (TILE, BLOCK))
            pivots[own] = jnp.where(row == sub, pivot, pivots[own])
            if j == PANEL - 1:
                break
            inverse = 1.0 / pivot
            factors = {}
            for r in range(own, tiles):
                value = columns[j][r] * inverse
                factors[r] = jnp.where(row > sub, value, 0.0) if r == own else value
            targets = columns[j + 1 :] + [panel]
            for target in targets:
                top = jnp.broadcast_to(target[own][sub : sub + 1, :], (TILE, BLOCK))
                for r in range(own, tiles):
                    target[r] = target[r] - factors[r] * top
        norm = jnp.concatenate([panel[r] * lax.rsqrt(pivots[r]) for r in range(tiles)], axis=0)
        wide = lax.broadcasted_iota(jnp.int32, (PANEL, BLOCK), 1)
        done.append(jnp.where(wide < start + PANEL, norm, 0.0))
        left = BLOCK - start - PANEL
        if left:
            update = dot(norm, norm, ((0,), (0,)))
            wide = lax.broadcasted_iota(jnp.int32, (left, BLOCK), 1)
            inside = (wide >= start) & (wide < start + PANEL)
            rest = jnp.where(inside, 0.0, rest[PANEL:, :]) - update[start + PANEL :, :]
    return jnp.concatenate(done, axis=0)


def factor_kernel(count, order_ref, packed_ref, out_ref, work):
    def piece(s, t):
        a, b = order_ref[s], order_ref[t]
        low, high = jnp.minimum(a, b), jnp.maximum(a, b)
        at = pl.multiple_of(slot(low, high, count) * BLOCK, BLOCK)
        value = packed_ref[pl.ds(at, BLOCK), :]
        return jnp.where(a <= b, value, value.T)

    def span(i):
        return slice(i * BLOCK, (i + 1) * BLOCK)

    def put(s, t, value):
        out_ref[
            pl.ds(pl.multiple_of(order_ref[s] * BLOCK, BLOCK), BLOCK),
            pl.ds(pl.multiple_of(order_ref[t] * BLOCK, BLOCK), BLOCK),
        ] = value

    for s, t in pairs(count):
        work[span(s), span(t)] = piece(s, t)

    for s in range(count):
        inverse = factor_block(work[span(s), span(s)])
        put(s, s, inverse)
        norm = {s: inverse}
        for t in range(s + 1, count):
            norm[t] = dot(inverse, work[span(s), span(t)], ((1,), (0,)))
        for r in range(s + 1, count):
            for t in range(r, count):
                work[span(r), span(t)] -= dot(norm[r], norm[t], ((0,), (0,)))
        for t in range(s):
            norm[t] = dot(inverse, work[span(s), span(t)], ((1,), (0,)))
            put(s, t, norm[t])
            put(t, s, jnp.zeros((BLOCK, BLOCK), jnp.float32))
        for r in range(s + 1, count):
            for t in range(s + 1):
                update = dot(norm[r], norm[t], ((0,), (0,)))
                work[span(r), span(t)] = -update if t == s else work[span(r), span(t)] - update


def factor_inverse(packed, order):
    count = order.shape[0]
    bands = count * BLOCK
    return pl.pallas_call(
        functools.partial(factor_kernel, count),
        out_shape=jax.ShapeDtypeStruct((bands, bands), jnp.float32),
        in_specs=[pl.BlockSpec(memory_space=pltpu.SMEM), pl.BlockSpec(memory_space=pltpu.VMEM)],
        out_specs=pl.BlockSpec(memory_space=pltpu.VMEM),
        scratch_shapes=[pltpu.VMEM((bands, bands), jnp.float32)],
    )(order, packed)


def solution(mesh):
    devices = mesh.shape["grid"]

    def local(psi, order):
        packed = packed_gram(psi, devices)
        inverse = factor_inverse(packed, order)
        return dot(psi, inverse, ((1,), (1,)))

    in_specs = (P(("frag", "grid"), None), P("frag"))
    out_specs = P(("frag", "grid"), None)
    return jax.shard_map(local, mesh=mesh, in_specs=in_specs, out_specs=out_specs, check_vma=False)
```

```python
import functools

import jax
import jax.numpy as jnp
from jax import lax
from jax.experimental import pallas as pl
from jax.experimental.pallas import tpu as pltpu
from jax.sharding import PartitionSpec as P

BLOCK = 128
PANEL = 16
TILE = 8
HIGHEST = lax.Precision.HIGHEST


def dot(left, right, dims):
    return lax.dot_general(
        left, right, (dims, ((), ())), precision=HIGHEST, preferred_element_type=jnp.float32
    )


def pairs(count):
    return [(i, j) for i in range(count) for j in range(i, count)]


def slot(i, j, count):
    return i * count - (i * (i - 1)) // 2 + (j - i)


def piece_ends(count, devices):
    unit, total, ends = devices * TILE, 0, [0]
    for i in range(count):
        total += (count - i) * BLOCK
        end = -(-total // unit) * unit
        if i != count - 2 and end > ends[-1]:
            ends.append(end)
    return ends


def gram_kernel(bits, scale, ends, psi_ref, out_ref, part, acc, recv, full, send_sem, recv_sem):
    me = lax.axis_index("grid")
    digit = [(me // 2**k) % 2 for k in range(bits)]
    partners = [me + (1 - 2 * digit[k]) * 2**k for k in range(bits)]
    rows = part.shape[0]
    count = psi_ref.shape[1] // BLOCK
    pieces = len(ends) - 1
    turn = 1 + (bits - 1) // 2
    routes = [
        list(range(bits)) if p % 2 == 0 else [0, *range(turn, bits), *range(1, turn)]
        for p in range(pieces)
    ]
    offset = ends[:-1]
    size = [ends[p + 1] - ends[p] for p in range(pieces)]
    base = ends[:-1]
    copies = [None] * pieces

    barrier = pltpu.get_barrier_semaphore()
    for partner in partners:
        pl.semaphore_signal(
            barrier, inc=1, device_id={"grid": partner}, device_id_type=pl.DeviceIdType.MESH
        )

    def send(p, src, dst, step, k):
        copies[p] = pltpu.make_async_remote_copy(
            src_ref=src,
            dst_ref=dst,
            send_sem=send_sem.at[p, step],
            recv_sem=recv_sem.at[p, step],
            device_id={"grid": partners[k]},
            device_id_type=pl.DeviceIdType.MESH,
        )
        copies[p].start()

    def scatter(p, step):
        k = routes[p][step]
        half = size[p] // 2
        give = pl.multiple_of(offset[p] + (1 - digit[k]) * half, TILE)
        source = part if step == 0 else acc
        send(p, source.at[pl.ds(give, half)], recv.at[pl.ds(base[p], half)], step, k)

    def reduce(p, step):
        k = routes[p][step]
        half = size[p] // 2
        keep = pl.multiple_of(offset[p] + digit[k] * half, TILE)
        copies[p].wait()
        source = part if step == 0 else acc
        target = full if step == bits - 1 else acc
        target[pl.ds(keep, half), :] = source[pl.ds(keep, half), :] + recv[base[p] : base[p] + half, :]
        offset[p], size[p], base[p] = keep, half, base[p] + half

    def gather(p, step):
        here = full.at[pl.ds(pl.multiple_of(offset[p], TILE), size[p])]
        send(p, here, here, bits + step, routes[p][step])

    def widen(p, step):
        copies[p].wait()
        offset[p] = offset[p] - digit[routes[p][step]] * size[p]
        size[p] *= 2

    at, begun = 0, 0
    for i in range(count):
        left = psi_ref[:, i * BLOCK : (i + 1) * BLOCK]
        row = dot(left, psi_ref[:, i * BLOCK :], ((0,), (0,))) * scale
        for j in range(i, count):
            part[at : at + BLOCK, :] = row[:, (j - i) * BLOCK : (j - i + 1) * BLOCK]
            at += BLOCK
        if i == count - 1 and at < rows:
            part[at:, :] = jnp.zeros((rows - at, BLOCK), jnp.float32)
            at = rows
        if i == 0:
            pl.semaphore_wait(barrier, bits)
        while begun < pieces and ends[begun + 1] <= at:
            scatter(begun, 0)
            begun += 1

    for step in range(bits):
        for p in range(pieces):
            reduce(p, step)
            if step < bits - 1:
                scatter(p, step + 1)
            else:
                gather(p, step)
    for step in reversed(range(bits)):
        for p in range(pieces):
            widen(p, step)
            if step > 0:
                gather(p, step - 1)
    out_ref[...] = full[: out_ref.shape[0], :]


def packed_gram(psi, devices):
    points, bands = psi.shape
    count = bands // BLOCK
    used = len(pairs(count)) * BLOCK
    ends = piece_ends(count, devices)
    bits = devices.bit_length() - 1
    scale = float(1.0 / (points * devices))
    buffer = pltpu.VMEM((ends[-1], BLOCK), jnp.float32)
    semaphores = pltpu.SemaphoreType.DMA((len(ends) - 1, 2 * bits))
    return pl.pallas_call(
        functools.partial(gram_kernel, bits, scale, ends),
        out_shape=jax.ShapeDtypeStruct((used, BLOCK), jnp.float32),
        in_specs=[pl.BlockSpec(memory_space=pltpu.VMEM)],
        out_specs=pl.BlockSpec(memory_space=pltpu.VMEM),
        scratch_shapes=[buffer, buffer, buffer, buffer, semaphores, semaphores],
        compiler_params=pltpu.CompilerParams(collective_id=0, has_side_effects=True),
    )(psi)


def factor_block(gram):
    tiles = PANEL // TILE
    row = lax.broadcasted_iota(jnp.int32, (TILE, BLOCK), 0)
    lane = lax.broadcasted_iota(jnp.int32, (TILE, BLOCK), 1)
    rest, done = gram, []
    for start in range(0, BLOCK, PANEL):
        panel = [rest[r * TILE : (r + 1) * TILE, :] for r in range(tiles)]
        columns = [
            [jnp.broadcast_to(panel[r][:, start + j : start + j + 1], (TILE, BLOCK)) for r in range(tiles)]
            for j in range(PANEL)
        ]
        inside = (lane >= start) & (lane < start + PANEL)
        panel = [
            jnp.where(inside, jnp.where(lane == row + (start + r * TILE), 1.0, 0.0), panel[r])
            for r in range(tiles)
        ]
        pivots = [jnp.ones((TILE, BLOCK), jnp.float32)] * tiles
        for j in range(PANEL):
            own, sub = divmod(j, TILE)
            pivot = jnp.broadcast_to(columns[j][own][sub : sub + 1, :], (TILE, BLOCK))
            pivots[own] = jnp.where(row == sub, pivot, pivots[own])
            if j == PANEL - 1:
                break
            inverse = 1.0 / pivot
            factors = {}
            for r in range(own, tiles):
                value = columns[j][r] * inverse
                factors[r] = jnp.where(row > sub, value, 0.0) if r == own else value
            targets = columns[j + 1 :] + [panel]
            for target in targets:
                top = jnp.broadcast_to(target[own][sub : sub + 1, :], (TILE, BLOCK))
                for r in range(own, tiles):
                    target[r] = target[r] - factors[r] * top
        norm = jnp.concatenate([panel[r] * lax.rsqrt(pivots[r]) for r in range(tiles)], axis=0)
        wide = lax.broadcasted_iota(jnp.int32, (PANEL, BLOCK), 1)
        done.append(jnp.where(wide < start + PANEL, norm, 0.0))
        left = BLOCK - start - PANEL
        if left:
            update = dot(norm, norm, ((0,), (0,)))
            wide = lax.broadcasted_iota(jnp.int32, (left, BLOCK), 1)
            inside = (wide >= start) & (wide < start + PANEL)
            rest = jnp.where(inside, 0.0, rest[PANEL:, :]) - update[start + PANEL :, :]
    return jnp.concatenate(done, axis=0)


def factor_kernel(count, order_ref, packed_ref, psi_ref, out_ref, work, x):
    def piece(s, t):
        a, b = order_ref[s], order_ref[t]
        low, high = jnp.minimum(a, b), jnp.maximum(a, b)
        at = pl.multiple_of(slot(low, high, count) * BLOCK, BLOCK)
        value = packed_ref[pl.ds(at, BLOCK), :]
        return jnp.where(a <= b, value, value.T)

    def span(i):
        return slice(i * BLOCK, (i + 1) * BLOCK)

    def home(s):
        return pl.ds(pl.multiple_of(order_ref[s] * BLOCK, BLOCK), BLOCK)

    for s, t in pairs(count):
        work[span(s), span(t)] = piece(s, t)
    for s in range(count):
        x[:, span(s)] = psi_ref[:, home(s)]

    for s in range(count):
        inverse = factor_block(work[span(s), span(s)])
        if s < count - 1:
            after = (s + 1) * BLOCK
            norm = dot(inverse, work[span(s), after:], ((1,), (0,)))
            for r in range(s + 1, count):
                skip = r * BLOCK - after
                left = norm[:, skip : skip + BLOCK]
                work[span(r), r * BLOCK :] -= dot(left, norm[:, skip:], ((0,), (0,)))
        q = dot(x[:, span(s)], inverse, ((1,), (1,)))
        out_ref[:, home(s)] = q
        if s < count - 1:
            x[:, after:] -= dot(q, norm, ((1,), (0,)))


def orthonormalize(packed, psi, order):
    count = order.shape[0]
    rows, bands = psi.shape
    vmem = pl.BlockSpec(memory_space=pltpu.VMEM)
    return pl.pallas_call(
        functools.partial(factor_kernel, count),
        out_shape=jax.ShapeDtypeStruct((rows, bands), jnp.float32),
        in_specs=[pl.BlockSpec(memory_space=pltpu.SMEM), vmem, vmem],
        out_specs=vmem,
        scratch_shapes=[
            pltpu.VMEM((bands, bands), jnp.float32),
            pltpu.VMEM((rows, bands), jnp.float32),
        ],
    )(order, packed, psi)


def solution(mesh):
    devices = mesh.shape["grid"]

    def local(psi, order):
        return orthonormalize(packed_gram(psi, devices), psi, order)

    in_specs = (P(("frag", "grid"), None), P("frag"))
    out_specs = P(("frag", "grid"), None)
    return jax.shard_map(local, mesh=mesh, in_specs=in_specs, out_specs=out_specs, check_vma=False)
```

```python
import functools

import jax
import jax.numpy as jnp
from jax import lax
from jax.experimental import pallas as pl
from jax.experimental.pallas import tpu as pltpu
from jax.sharding import PartitionSpec as P

BLOCK = 128
PANEL = 16
TILE = 8
HIGHEST = lax.Precision.HIGHEST


def dot(left, right, dims):
    return lax.dot_general(
        left, right, (dims, ((), ())), precision=HIGHEST, preferred_element_type=jnp.float32
    )


def pairs(count):
    return [(i, j) for i in range(count) for j in range(i, count)]


def slot(i, j, count):
    return i * count - (i * (i - 1)) // 2 + (j - i)


def piece_ends(count, devices):
    unit, total, ends = devices * TILE, 0, [0]
    for i in range(count):
        total += (count - i) * BLOCK
        end = -(-total // unit) * unit
        if i != count - 2 and end > ends[-1]:
            ends.append(end)
    return ends


def gram_kernel(bits, scale, ends, psi_ref, out_ref, part, acc, recv, full, send_sem, recv_sem):
    me = lax.axis_index("grid")
    digit = [(me // 2**k) % 2 for k in range(bits)]
    partners = [me + (1 - 2 * digit[k]) * 2**k for k in range(bits)]
    rows = part.shape[0]
    count = psi_ref.shape[1] // BLOCK
    pieces = len(ends) - 1
    turn = 1 + (bits - 1) // 2
    routes = [
        list(range(bits)) if p % 2 == 0 else [0, *range(turn, bits), *range(1, turn)]
        for p in range(pieces)
    ]
    offset = ends[:-1]
    size = [ends[p + 1] - ends[p] for p in range(pieces)]
    base = ends[:-1]
    copies = [None] * pieces

    barrier = pltpu.get_barrier_semaphore()
    for partner in partners:
        pl.semaphore_signal(
            barrier, inc=1, device_id={"grid": partner}, device_id_type=pl.DeviceIdType.MESH
        )

    def send(p, src, dst, step, k):
        copies[p] = pltpu.make_async_remote_copy(
            src_ref=src,
            dst_ref=dst,
            send_sem=send_sem.at[p, step],
            recv_sem=recv_sem.at[p, step],
            device_id={"grid": partners[k]},
            device_id_type=pl.DeviceIdType.MESH,
        )
        copies[p].start()

    def scatter(p, step):
        k = routes[p][step]
        half = size[p] // 2
        give = pl.multiple_of(offset[p] + (1 - digit[k]) * half, TILE)
        source = part if step == 0 else acc
        send(p, source.at[pl.ds(give, half)], recv.at[pl.ds(base[p], half)], step, k)

    def reduce(p, step):
        k = routes[p][step]
        half = size[p] // 2
        keep = pl.multiple_of(offset[p] + digit[k] * half, TILE)
        copies[p].wait()
        source = part if step == 0 else acc
        target = full if step == bits - 1 else acc
        target[pl.ds(keep, half), :] = source[pl.ds(keep, half), :] + recv[base[p] : base[p] + half, :]
        offset[p], size[p], base[p] = keep, half, base[p] + half

    def gather(p, step):
        here = full.at[pl.ds(pl.multiple_of(offset[p], TILE), size[p])]
        send(p, here, here, bits + step, routes[p][step])

    def widen(p, step):
        copies[p].wait()
        offset[p] = offset[p] - digit[routes[p][step]] * size[p]
        size[p] *= 2

    at, begun = 0, 0
    for i in range(count):
        left = psi_ref[:, i * BLOCK : (i + 1) * BLOCK]
        row = dot(left, psi_ref[:, i * BLOCK :], ((0,), (0,))) * scale
        for j in range(i, count):
            part[at : at + BLOCK, :] = row[:, (j - i) * BLOCK : (j - i + 1) * BLOCK]
            at += BLOCK
        if i == count - 1 and at < rows:
            part[at:, :] = jnp.zeros((rows - at, BLOCK), jnp.float32)
            at = rows
        if i == 0:
            pl.semaphore_wait(barrier, bits)
        while begun < pieces and ends[begun + 1] <= at:
            scatter(begun, 0)
            begun += 1

    for step in range(bits):
        for p in range(pieces):
            reduce(p, step)
            if step < bits - 1:
                scatter(p, step + 1)
            else:
                gather(p, step)
    for step in reversed(range(bits)):
        for p in range(pieces):
            widen(p, step)
            if step > 0:
                gather(p, step - 1)
    out_ref[...] = full[: out_ref.shape[0], :]


def packed_gram(psi, devices):
    points, bands = psi.shape
    count = bands // BLOCK
    used = len(pairs(count)) * BLOCK
    ends = piece_ends(count, devices)
    bits = devices.bit_length() - 1
    scale = float(1.0 / (points * devices))
    buffer = pltpu.VMEM((ends[-1], BLOCK), jnp.float32)
    semaphores = pltpu.SemaphoreType.DMA((len(ends) - 1, 2 * bits))
    return pl.pallas_call(
        functools.partial(gram_kernel, bits, scale, ends),
        out_shape=jax.ShapeDtypeStruct((used, BLOCK), jnp.float32),
        in_specs=[pl.BlockSpec(memory_space=pltpu.VMEM)],
        out_specs=pl.BlockSpec(memory_space=pltpu.VMEM),
        scratch_shapes=[buffer, buffer, buffer, buffer, semaphores, semaphores],
        compiler_params=pltpu.CompilerParams(collective_id=0, has_side_effects=True),
    )(psi)


def thirds(value):
    high = value.astype(jnp.bfloat16)
    value = value - high.astype(jnp.float32)
    middle = value.astype(jnp.bfloat16)
    return high, middle, (value - middle.astype(jnp.float32)).astype(jnp.bfloat16)


def factor_block(gram):
    tiles = PANEL // TILE
    row = lax.broadcasted_iota(jnp.int32, (TILE, BLOCK), 0)
    lane = lax.broadcasted_iota(jnp.int32, (TILE, BLOCK), 1)
    rest, done = gram, []
    for start in range(0, BLOCK, PANEL):
        panel = [rest[r * TILE : (r + 1) * TILE, :] for r in range(tiles)]
        columns = [
            [jnp.broadcast_to(panel[r][:, start + j : start + j + 1], (TILE, BLOCK)) for r in range(tiles)]
            for j in range(PANEL)
        ]
        inside = (lane >= start) & (lane < start + PANEL)
        panel = [
            jnp.where(inside, jnp.where(lane == row + (start + r * TILE), 1.0, 0.0), panel[r])
            for r in range(tiles)
        ]
        pivots = [jnp.ones((TILE, BLOCK), jnp.float32)] * tiles
        for j in range(PANEL):
            own, sub = divmod(j, TILE)
            pivot = jnp.broadcast_to(columns[j][own][sub : sub + 1, :], (TILE, BLOCK))
            pivots[own] = jnp.where(row == sub, pivot, pivots[own])
            if j == PANEL - 1:
                break
            inverse = 1.0 / pivot
            factors = {}
            for r in range(own, tiles):
                value = columns[j][r] * inverse
                factors[r] = jnp.where(row > sub, value, 0.0) if r == own else value
            targets = columns[j + 1 :] + [panel]
            for target in targets:
                top = jnp.broadcast_to(target[own][sub : sub + 1, :], (TILE, BLOCK))
                for r in range(own, tiles):
                    target[r] = target[r] - factors[r] * top
        norm = jnp.concatenate([panel[r] * lax.rsqrt(pivots[r]) for r in range(tiles)], axis=0)
        wide = lax.broadcasted_iota(jnp.int32, (PANEL, BLOCK), 1)
        done.append(jnp.where(wide < start + PANEL, norm, 0.0))
        left = BLOCK - start - PANEL
        if left:
            high, middle, low = thirds(norm)
            left_parts = jnp.concatenate([low, high, middle, middle, high, high], axis=0)
            right_parts = jnp.concatenate([high, low, middle, high, middle, high], axis=0)
            turned = left_parts.T
            cuts = [start + PANEL, start + 2 * PANEL, BLOCK]
            update = jnp.concatenate(
                [
                    jnp.dot(turned[a:b, :], right_parts, preferred_element_type=jnp.float32)
                    for a, b in zip(cuts, cuts[1:])
                    if a < b
                ],
                axis=0,
            )
            wide = lax.broadcasted_iota(jnp.int32, (left, BLOCK), 1)
            inside = (wide >= start) & (wide < start + PANEL)
            rest = jnp.where(inside, 0.0, rest[PANEL:, :]) - update
    return jnp.concatenate(done, axis=0)


def factor_kernel(count, order_ref, packed_ref, psi_ref, out_ref, work, x):
    def piece(s, t):
        a, b = order_ref[s], order_ref[t]
        low, high = jnp.minimum(a, b), jnp.maximum(a, b)
        at = pl.multiple_of(slot(low, high, count) * BLOCK, BLOCK)
        value = packed_ref[pl.ds(at, BLOCK), :]
        return jnp.where(a <= b, value, value.T)

    def span(i):
        return slice(i * BLOCK, (i + 1) * BLOCK)

    def home(s):
        return pl.ds(pl.multiple_of(order_ref[s] * BLOCK, BLOCK), BLOCK)

    for s, t in pairs(count):
        work[span(s), span(t)] = piece(s, t)
    for s in range(count):
        x[:, span(s)] = psi_ref[:, home(s)]

    for s in range(count):
        inverse = factor_block(work[span(s), span(s)])
        if s < count - 1:
            after = (s + 1) * BLOCK
            norm = dot(inverse, work[span(s), after:], ((1,), (0,)))
            for r in range(s + 1, count):
                skip = r * BLOCK - after
                left = norm[:, skip : skip + BLOCK]
                work[span(r), r * BLOCK :] -= dot(left, norm[:, skip:], ((0,), (0,)))
        q = dot(x[:, span(s)], inverse, ((1,), (1,)))
        out_ref[:, home(s)] = q
        if s < count - 1:
            x[:, after:] -= dot(q, norm, ((1,), (0,)))


def orthonormalize(packed, psi, order):
    count = order.shape[0]
    rows, bands = psi.shape
    vmem = pl.BlockSpec(memory_space=pltpu.VMEM)
    return pl.pallas_call(
        functools.partial(factor_kernel, count),
        out_shape=jax.ShapeDtypeStruct((rows, bands), jnp.float32),
        in_specs=[pl.BlockSpec(memory_space=pltpu.SMEM), vmem, vmem],
        out_specs=vmem,
        scratch_shapes=[
            pltpu.VMEM((bands, bands), jnp.float32),
            pltpu.VMEM((rows, bands), jnp.float32),
        ],
    )(order, packed, psi)


def solution(mesh):
    devices = mesh.shape["grid"]

    def local(psi, order):
        return orthonormalize(packed_gram(psi, devices), psi, order)

    in_specs = (P(("frag", "grid"), None), P("frag"))
    out_specs = P(("frag", "grid"), None)
    return jax.shard_map(local, mesh=mesh, in_specs=in_specs, out_specs=out_specs, check_vma=False)
```
